32 devices in a mesh: expert: 16 (over z, y, x), vocab: 2 (over core).
Axes of the slice: x: 2, y: 2, z: 4, core: 2. Of those that a mesh axis runs over, the one named last changes fastest.
Arguments:
- out_grad: bfloat16 [2048, 4096], P('expert', 'vocab'), may hold values from -6 to 6
- residual_stream: bfloat16 [2048, 4096], P('expert', 'vocab'), may hold values from -228 to 228
- norm_gain: float32 [4096], P('vocab'), may hold values from 0.25 to 51
- expert_ids: int32 [2048, 8], P('expert'), may hold values from 0 to 15, all different within a row; in each aligned block of 128 rows (0 to 127, 128 to 255, ...) at most 76 rows name the same one
- gate_scores: float32 [2048, 8], P('expert'), may hold values from 0.05 to 1
- saved_gate: bfloat16 [16, 1216, 1536], P('expert', None, 'vocab'), may hold values from -6 to 6
- saved_up: bfloat16 [16, 1216, 1536], P('expert', None, 'vocab'), may hold values from -6 to 6
- gate_weight: bfloat16 [16, 4096, 1536], P('expert', None, 'vocab'), may hold values from -0.09375 to 0.09375
- up_weight: bfloat16 [16, 4096, 1536], P('expert', None, 'vocab'), may hold values from -0.09375 to 0.09375
- down_weight: bfloat16 [16, 1536, 4096], P('expert', 'vocab'), may hold values from -0.15625 to 0.15625
- embedding: bfloat16 [12288, 4096], P(('expert', 'vocab')), may hold values from -0.09375 to 0.09375
- allowed: int32 [12288], P(('expert', 'vocab')), may hold values 0 or 1
- suffix_start: int32 [16], P('expert'), may hold values from 0 to 108
Outputs:
- token_grad: bfloat16 [2048, 4096], P('expert', 'vocab')
- scores: float32 [320, 12288], P(None, ('expert', 'vocab'))
The draws below stay inside these ranges and needn't reach their ends.
Inputs may be any that keep to these rules, and one draw needn't show every extreme that they name: `expert_ids`: in each aligned block of 128 rows (one behavior) a row names 8 different experts and no expert is named by more than 76 rows; some expert is named by exactly 76 rows in some blocks.
All inputs are finite; a program needn't handle non-finite values. No bound on the sum of `allowed` on one device may be relied on, other than what follows from the above.
Results may differ from the reference program's by a relative error of at most 0.01.
Values may be sent and summed in bfloat16 or wider, within the bound.
A program may use at most 128 MiB of HBM per device.

```python
import math
import jax
import jax.numpy as jnp
import numpy as np
from jax import lax

D = 4096
FF = 1536
TOP = 8
SEQ = 128
SUFFIX = 20
EXPERTS = 16
BEHAVIORS = 16
TOKENS = 2048
CAP = 76
SLOTS = 1216
VOCAB = 12288
N_EXPERT = 16
N_VOCAB = 2


massive_count = 4


def massive_mask(key):
    order = jax.random.permutation(jax.random.fold_in(key, 101), D)
    picked = order[:massive_count]
    return jnp.zeros((D,), jnp.float32).at[picked].set(1.0) > 0.5


def draw_residual_stream(key, part):
    key_base, key_rows, key_big, key_sign = jax.random.split(jax.random.fold_in(key, 7), 4)
    columns = jnp.exp(math.log(3.0) * jnp.arange(D, dtype=jnp.float32) / D)
    base = jnp.clip(jax.random.normal(key_base, (TOKENS, D), jnp.float32), -5.0, 5.0)
    bulk = base * columns[None, :]
    amplitude = jnp.sqrt(jnp.mean(columns * columns) * D / massive_count)
    magnitude = jax.random.uniform(key_big, (TOKENS, D), jnp.float32, 0.7, 1.4)
    signs = jnp.where(jax.random.bernoulli(key_sign, 0.5, (TOKENS, D)), 1.0, -1.0)
    strong = amplitude * magnitude * signs
    mask = massive_mask(key)
    values = jnp.where(mask[None, :], strong, bulk)
    row_scale = jnp.exp(jax.random.uniform(key_rows, (TOKENS, 1), jnp.float32, math.log(0.1), math.log(1.0)))
    return (values * row_scale).astype(jnp.bfloat16)


def draw_norm_gain(key, part):
    key_base, key_big = jax.random.split(jax.random.fold_in(key, 13))
    base = 1.0 + 0.18 * jnp.clip(jax.random.normal(key_base, (D,), jnp.float32), -4.0, 4.0)
    strong = jnp.sqrt(jnp.float32(D) / massive_count) * jax.random.uniform(key_big, (D,), jnp.float32, 0.7, 1.4)
    mask = massive_mask(key)
    return jnp.where(mask, strong, base).astype(jnp.float32)


def touch_ends(entries, rng, low, top_value):
    dims = entries.shape
    place = [jax.random.randint(jax.random.fold_in(rng, axis), (), 0, dims[axis]) for axis in range(len(dims))]
    entries = entries.at[tuple(place)].set(low)
    longest = dims.index(max(dims))
    place[longest] = (place[longest] + 1) % dims[longest]
    return entries.at[tuple(place)].set(top_value)


def level_of(stream_key, extent, cuts, smallest, top_value):
    factor_of = 1.0
    for axis_at, blocks in cuts:
        steps = jax.random.uniform(jax.random.fold_in(jax.random.fold_in(stream_key, 6), axis_at), (blocks,), jnp.float32, smallest / len(cuts), top_value / len(cuts))
        factor_of = factor_of * jnp.repeat(jnp.exp(steps), extent[axis_at] // blocks).reshape((-1,) + (1,) * (len(extent) - 1 - axis_at))
    return factor_of


def deal_out(rng, own, number, rows, count, top, bound, slope):
    sequence = jax.random.permutation(rng, count)
    packed, common = load_shares(count, rows * top, bound, slope, True), load_shares(count, rows * top, bound, slope, False)
    places = jnp.arange(count)

    def named(tallies, offset_by):
        used = int((tallies > 0).sum())
        fixed = max(1, used // 4)
        shifted = fixed + (places - fixed + offset_by * (used - fixed)) % max(1, count - fixed)
        return jnp.zeros((count,), jnp.int32).at[sequence[jnp.where(places < fixed, places, shifted)]].set(jnp.asarray(tallies, jnp.int32))

    tallies = jnp.where(number % 4 == 0, named(packed, number // 4), named(common, number - number // 4 - 1))
    mixed = jax.random.permutation(jax.random.fold_in(own, 3), count)
    source_of, receiver = mixed[0:count // 2 * 2:2], mixed[1:count // 2 * 2:2]
    room = jnp.minimum(tallies[source_of] - 1, bound - tallies[receiver]) // 2
    room = jnp.where((source_of == sequence[0]) | (receiver == sequence[0]) | (tallies[receiver] == 0), 0, jnp.maximum(room, 0))
    shifted = jax.random.randint(jax.random.fold_in(own, 4), (count // 2,), 0, 1 << 20) % (room + 1)
    tallies = tallies.at[source_of].add(-shifted).at[receiver].add(shifted)
    items = jnp.searchsorted(jnp.cumsum(tallies), jnp.arange(rows * top), side="right").astype(jnp.int32)
    listing = items.reshape(top, rows).T
    listing = listing[jax.random.permutation(jax.random.fold_in(own, 1), rows)]
    offset_by = jax.random.randint(jax.random.fold_in(own, 2), (rows, 1), 0, top)
    return jnp.take_along_axis(listing, (jnp.arange(top)[None, :] + offset_by) % top, axis=1)


def load_shares(number_of, total, most, skew, full):
    weights = [(1 << 20) // math.isqrt(standing ** skew) + 1 for standing in range(1, number_of + 1)]
    largest = most if full else min(most, max(-(-total // number_of), total * weights[0] // sum(weights)))
    least = 1 if total - largest >= number_of - 1 else 0
    given, spare = [largest] + [least] * (number_of - 1), total - largest - least * (number_of - 1)
    while spare > 0:
        candidates = [i for i in range(1, number_of) if given[i] < largest] or [i for i in range(1, number_of) if given[i] < most]
        pool, left = sum([weights[i] for i in candidates]), spare
        for i in candidates:
            more = min(most - given[i], max(1, left * weights[i] // pool), spare)
            given[i] = given[i] + more
            spare = spare - more
    return np.array(given)


def gaussian(own_key, shape, width, bound, cuts=(), kind=jnp.bfloat16):
    loudness = level_of(own_key, shape, cuts, -0.22, 0.18) if cuts else 1.0
    entries = jax.random.normal(own_key, shape, jnp.float32) * width * loudness
    return jnp.minimum(jnp.maximum(entries, -bound), bound).astype(kind)


def setup_inputs(seed: int = 0) -> dict:
    key_of = jax.random.split(jax.random.key(seed), 14)
    out_grad = gaussian(key_of[0], (TOKENS, D), 1.0, 6.0, ((0, 16), (1, 2)))
    residual_stream = draw_residual_stream(jax.random.fold_in(key_of[13], 71), 0)
    norm_gain = draw_norm_gain(jax.random.fold_in(key_of[13], 71), 0)
    expert_ids_keys = jax.random.split(jax.random.fold_in(key_of[3], 1), TOKENS // SEQ)
    expert_ids_turns = jax.random.permutation(jax.random.fold_in(key_of[3], 3), TOKENS // SEQ)
    expert_ids = jax.vmap(lambda own, number: deal_out(jax.random.fold_in(key_of[3], 2), own, number, SEQ, EXPERTS, TOP, CAP, 2))(expert_ids_keys, expert_ids_turns).reshape((TOKENS, TOP))
    gate_scores = jnp.clip(jnp.exp(math.log(1.0) - 2.9957323 * jax.random.uniform(key_of[4], (TOKENS, TOP), jnp.float32) ** level_of(key_of[4], (TOKENS, TOP), ((0, 16),), -0.2, 0.2)), 0.05, 1.0)
    saved_gate = gaussian(key_of[5], (EXPERTS, SLOTS, FF), 1.0, 6.0, ((0, 16), (2, 2)))
    saved_up = gaussian(key_of[6], (EXPERTS, SLOTS, FF), 1.0, 6.0, ((0, 16), (2, 2)))
    gate_weight = gaussian(key_of[7], (EXPERTS, D, FF), D ** -0.5, 0.09375, ((0, 16), (2, 2)))
    up_weight = gaussian(key_of[8], (EXPERTS, D, FF), D ** -0.5, 0.09375, ((0, 16), (2, 2)))
    down_weight = gaussian(key_of[9], (EXPERTS, FF, D), FF ** -0.5, 0.15625, ((0, 16), (1, 2)))
    embedding = gaussian(key_of[10], (VOCAB, D), D ** -0.5, 0.09375, ((0, 32),))
    allowed = touch_ends((jax.random.randint(key_of[11], (VOCAB,), 0, 4) < 3).astype(jnp.int32), jax.random.fold_in(key_of[11], 1), 0, 1)
    suffix_start = touch_ends(jax.random.randint(key_of[12], (BEHAVIORS,), 0, SEQ - SUFFIX + 1), jax.random.fold_in(key_of[12], 1), 0, SEQ - SUFFIX).astype(jnp.int32)
    return dict(out_grad=out_grad, residual_stream=residual_stream, norm_gain=norm_gain, expert_ids=expert_ids, gate_scores=gate_scores, saved_gate=saved_gate, saved_up=saved_up, gate_weight=gate_weight, up_weight=up_weight, down_weight=down_weight, embedding=embedding, allowed=allowed, suffix_start=suffix_start)


def slot_places(expert_ids):
    blocks = expert_ids.reshape(N_EXPERT, SEQ * TOP)
    matches = (blocks[:, :, None] == jnp.arange(EXPERTS, dtype=jnp.int32)[None, None, :]).astype(jnp.int32)
    before = jnp.cumsum(matches, axis=1) - matches
    position = lax.optimization_barrier(jnp.sum(before * matches, axis=2)).astype(jnp.int32)
    source = jnp.arange(N_EXPERT, dtype=jnp.int32)[:, None]
    slot = (source * CAP + position).astype(jnp.int32)
    return (blocks.reshape(-1), slot.reshape(-1))

def reference(out_grad, residual_stream, norm_gain, expert_ids, gate_scores, saved_gate, saved_up, gate_weight, up_weight, down_weight, embedding, allowed, suffix_start):
    gate_share = gate_scores / lax.optimization_barrier(jnp.sum(gate_scores, axis=1, keepdims=True))
    chosen, slot = slot_places(expert_ids)
    token_of = (jnp.arange(TOKENS * TOP, dtype=jnp.int32) // TOP).astype(jnp.int32)
    owner = jnp.full((EXPERTS, SLOTS), TOKENS, jnp.int32).at[chosen, slot].set(token_of)
    share_of = jnp.zeros((EXPERTS, SLOTS), jnp.float32).at[chosen, slot].set(gate_share.reshape(-1))
    grad_ext = jnp.concatenate([out_grad.astype(jnp.float32), jnp.zeros((1, D), jnp.float32)], axis=0)
    group = FF // N_VOCAB

    def expert_step(accumulated, pieces):
        rows, slot_gate, pre_gate, pre_up, w_gate, w_up, w_down = pieces
        routed = (slot_gate[:, None] * grad_ext[rows]).astype(jnp.bfloat16)
        act_grad = jnp.dot(routed, w_down.T, preferred_element_type=jnp.float32)
        pre_gate = pre_gate.astype(jnp.float32)
        pre_up = pre_up.astype(jnp.float32)
        sigmoid_g = jax.nn.sigmoid(pre_gate)
        gate_grad = (act_grad * pre_up * sigmoid_g * (1.0 + pre_gate * (1.0 - sigmoid_g))).astype(jnp.bfloat16)
        up_grad = (act_grad * pre_gate * sigmoid_g).astype(jnp.bfloat16)
        gate_split = gate_grad.astype(jnp.float32).reshape(SLOTS, N_VOCAB, group)
        up_split = up_grad.astype(jnp.float32).reshape(SLOTS, N_VOCAB, group)
        wg_split = w_gate.astype(jnp.float32).reshape(D, N_VOCAB, group)
        wu_split = w_up.astype(jnp.float32).reshape(D, N_VOCAB, group)
        partial_value = jnp.einsum('rvh,dvh->vrd', gate_split, wg_split) + jnp.einsum('rvh,dvh->vrd', up_split, wu_split)
        rounded = lax.optimization_barrier(partial_value.astype(jnp.bfloat16))
        slot_grad = lax.optimization_barrier(jnp.sum(rounded.astype(jnp.float32), axis=0))
        accumulated = accumulated.at[rows].add(slot_grad, mode='drop')
        return (accumulated, None)
    moe_grad, _ = lax.scan(expert_step, jnp.zeros((TOKENS, D), jnp.float32), (owner, share_of, saved_gate, saved_up, gate_weight, up_weight, down_weight))
    resid = residual_stream.astype(jnp.float32)
    inverse = lax.rsqrt(lax.optimization_barrier(jnp.mean(resid * resid, axis=1)) + 1e-06)
    normed = resid * inverse[:, None]
    scaled = moe_grad * norm_gain[None, :]
    project = lax.optimization_barrier(jnp.mean(scaled * normed, axis=1))
    token_grad = (out_grad.astype(jnp.float32) + inverse[:, None] * (scaled - normed * project[:, None])).astype(jnp.bfloat16)
    per_behavior = token_grad.reshape(N_EXPERT, SEQ, D)

    def take_suffix(rows, first_row):
        return lax.dynamic_slice_in_dim(rows, first_row.astype(jnp.int32), SUFFIX, 0)
    suffix_grad = jax.vmap(take_suffix)(per_behavior, suffix_start).reshape(N_EXPERT * SUFFIX, D)
    raw_scores = -jnp.dot(suffix_grad, embedding.T, preferred_element_type=jnp.float32)
    scores = jnp.where(allowed[None, :] > 0, raw_scores, jnp.float32(0.0))
    return (token_grad, scores)
```

```python
import functools

import jax
import jax.numpy as jnp
from jax import lax
from jax.experimental import pallas as pl
from jax.experimental.pallas import tpu as pltpu
from jax.sharding import PartitionSpec as P

D = 4096
SUFFIX = 20
MESH = pl.DeviceIdType.MESH


def dispatch_kernel(n, nv, src, out, here, send, recv, fsend, frecv):
    e, v = lax.axis_index("expert"), lax.axis_index("vocab")
    width = src.shape[2]

    def block_for(to):
        return src.at[to if src.shape[0] > 1 else 0]

    def place(row, col):
        return out.at[row, :, pl.ds(pl.multiple_of(col * width, 128), width)]

    local = pltpu.make_async_copy(block_for(e), place(e, v), here)
    local.start()

    def pass_on(j, i, block):
        row = lax.rem(e - j + n, n)
        return pltpu.make_async_remote_copy(
            src_ref=block,
            dst_ref=place(row, v),
            send_sem=fsend.at[j, i - 1],
            recv_sem=frecv.at[j, i - 1],
            device_id=(e, lax.rem(v + i, nv)),
            device_id_type=MESH,
        )

    def across(j):
        to = lax.rem(e + j, n)
        return pltpu.make_async_remote_copy(
            src_ref=block_for(to),
            dst_ref=place(e, v),
            send_sem=send.at[j],
            recv_sem=recv.at[j],
            device_id=(to, v),
            device_id_type=MESH,
        )

    for j in range(1, n):
        across(j).start()
    for i in range(1, nv):
        pass_on(0, i, block_for(e)).start()
    for j in range(1, n):
        across(j).wait_recv()
        for i in range(1, nv):
            pass_on(j, i, place(lax.rem(e - j + n, n), v)).start()
    for j in range(n):
        for i in range(1, nv):
            pass_on(j, i, block_for(e)).wait()
    for j in range(1, n):
        across(j).wait_send()
    local.wait()


def dispatch(blocks, n, nv):
    _, rows, width = blocks.shape
    return pl.pallas_call(
        functools.partial(dispatch_kernel, n, nv),
        out_shape=jax.ShapeDtypeStruct((n, rows, width * nv), blocks.dtype),
        in_specs=[pl.BlockSpec(memory_space=pl.ANY)],
        out_specs=pl.BlockSpec(memory_space=pl.ANY),
        scratch_shapes=[
            pltpu.SemaphoreType.DMA,
            pltpu.SemaphoreType.DMA((n,)),
            pltpu.SemaphoreType.DMA((n,)),
            pltpu.SemaphoreType.DMA((n, nv - 1)),
            pltpu.SemaphoreType.DMA((n, nv - 1)),
        ],
        compiler_params=pltpu.CompilerParams(has_side_effects=True),
    )(blocks)


def shards(
    out_grad,
    residual_stream,
    norm_gain,
    expert_ids,
    gate_scores,
    saved_gate,
    saved_up,
    gate_weight,
    up_weight,
    down_weight,
    embedding,
    allowed,
    suffix_start,
):
    n_expert = lax.axis_size("expert")
    seq_len, d_slice = out_grad.shape
    n_vocab = lax.axis_size("vocab")
    slot_count = saved_gate.shape[1]
    capacity = slot_count // n_expert
    padded = -(-capacity // 16) * 16
    contract = (((1,), (1,)), ((), ()))
    experts = jnp.arange(n_expert, dtype=jnp.int32)
    gate_share = gate_scores / jnp.sum(gate_scores, axis=1, keepdims=True)
    named = expert_ids[:, :, None] == experts
    chosen = jnp.any(named, axis=1)
    share = jnp.sum(jnp.where(named, gate_share[:, :, None], 0.0), axis=1)
    tokens = jnp.arange(seq_len, dtype=jnp.int32)
    earlier = (tokens[None, :] < tokens[:, None]).astype(jnp.bfloat16)
    position = jnp.dot(
        earlier, chosen.astype(jnp.bfloat16), preferred_element_type=jnp.float32
    ).astype(jnp.int32)
    position = jnp.where(chosen, position, -1).T
    holds = position[:, None, :] == jnp.arange(padded, dtype=jnp.int32)[None, :, None]
    share_of = jnp.sum(jnp.where(holds, share.T[:, None, :], 0.0), axis=2)
    pick = holds.astype(jnp.bfloat16).reshape(n_expert * padded, seq_len)
    taken = jnp.dot(pick, out_grad, preferred_element_type=jnp.float32)
    routed = (share_of.reshape(-1, 1) * taken).astype(jnp.bfloat16)
    incoming = dispatch(routed.reshape(n_expert, padded, d_slice), n_expert, n_vocab)
    incoming = incoming.reshape(n_expert * padded, d_slice * n_vocab)

    def widen(saved):
        wide = saved.reshape(n_expert, capacity, -1)
        wide = jnp.pad(wide, ((0, 0), (0, padded - capacity), (0, 0)))
        return wide.reshape(n_expert * padded, -1).astype(jnp.float32)

    act_grad = lax.dot_general(
        incoming, down_weight[0], contract, preferred_element_type=jnp.float32
    )
    pre_gate = widen(saved_gate[0])
    pre_up = widen(saved_up[0])
    sigmoid_g = jax.nn.sigmoid(pre_gate)
    gate_grad = (act_grad * pre_up * sigmoid_g * (1.0 + pre_gate * (1.0 - sigmoid_g))).astype(
        jnp.bfloat16
    )
    up_grad = (act_grad * pre_gate * sigmoid_g).astype(jnp.bfloat16)
    partial_value = lax.dot_general(
        gate_grad, gate_weight[0], contract, preferred_element_type=jnp.float32
    )
    partial_value = partial_value + lax.dot_general(
        up_grad, up_weight[0], contract, preferred_element_type=jnp.float32
    )
    partial_rounded = partial_value.astype(jnp.bfloat16)
    slot_grad = lax.psum_scatter(partial_rounded, "vocab", scatter_dimension=1, tiled=True)
    returned = lax.all_to_all(
        slot_grad.reshape(n_expert, padded, d_slice),
        "expert",
        split_axis=0,
        concat_axis=0,
        tiled=True,
    ).reshape(n_expert * padded, d_slice)
    moe_grad = lax.dot_general(
        pick, returned, (((0,), (0,)), ((), ())), preferred_element_type=jnp.float32
    )
    resid = residual_stream.astype(jnp.float32)
    scaled = moe_grad * norm_gain[None, :]
    sums = lax.psum(
        jnp.stack([jnp.sum(resid * resid, axis=1), jnp.sum(scaled * resid, axis=1)]), "vocab"
    )
    inverse = lax.rsqrt(sums[0] / D + 1e-06)
    normed = resid * inverse[:, None]
    row_project = inverse * (sums[1] / D)
    token_grad = (
        out_grad.astype(jnp.float32) + inverse[:, None] * (scaled - normed * row_project[:, None])
    ).astype(jnp.bfloat16)
    suffix_grad = lax.dynamic_slice_in_dim(token_grad, suffix_start[0], SUFFIX, 0)
    suffix_rows = -(-SUFFIX // 16) * 16
    suffix_grad = jnp.pad(suffix_grad, ((0, suffix_rows - SUFFIX), (0, 0)))
    suffix_grad = dispatch(suffix_grad[None], n_expert, n_vocab)[:, :SUFFIX]
    raw_scores = -lax.dot_general(
        suffix_grad.reshape(n_expert * SUFFIX, d_slice * n_vocab),
        embedding,
        contract,
        preferred_element_type=jnp.float32,
    )
    scores = jnp.where(allowed[None, :] > 0, raw_scores, jnp.float32(0.0))
    return (token_grad, scores)


def solution(mesh):
    placed = (
        P("expert", "vocab"),
        P("expert", "vocab"),
        P("vocab"),
        P("expert", None),
        P("expert", None),
        P("expert", None, "vocab"),
        P("expert", None, "vocab"),
        P("expert", None, "vocab"),
        P("expert", None, "vocab"),
        P("expert", "vocab", None),
        P(("expert", "vocab"), None),
        P(("expert", "vocab")),
        P("expert"),
    )
    return jax.shard_map(
        shards,
        mesh=mesh,
        in_specs=placed,
        out_specs=(P("expert", "vocab"), P(None, ("expert", "vocab"))),
        check_vma=False,
    )
```
